256 devices in a mesh: row: 16 (over x_lo, y, core), col: 16 (over z, x_hi).
Axes of the slice: x: 4 (x_hi: 2, x_lo: 2; x = x_hi * 2 + x_lo), y: 4, z: 8, core: 2. Of those that a mesh axis runs over, the one named last changes fastest.
Arguments:
- species: bfloat16 [3, 512, 512, 256], P(None, 'row', 'col'), may hold values from -6 to 6
- flow_field: bfloat16 [3, 512, 512, 256], P(None, 'row', 'col'), may hold values from -6 to 6
- x_operators: bfloat16 [2, 512, 512], replicated, may hold values from -8 to 8
- y_operators: bfloat16 [2, 512, 512], replicated, may hold values from -8 to 8
Outputs:
- species_derivatives: bfloat16 [3, 2, 512, 512, 256], P(None, None, 'row', 'col')
- flow_derivatives: bfloat16 [3, 2, 512, 512, 256], P(None, None, 'row', 'col')
The draws below stay inside these ranges and needn't reach their ends.
All inputs are finite; a program needn't handle non-finite values.
Results may differ from the reference program's by a relative error of at most 0.001.
Values may be sent and summed in bfloat16 or wider, within the bound.
No kernel may reach another device: no remote copies, remote signals or barrier semaphores. Data moves between devices by JAX's collectives and lax.ppermute only.
A program may use at most 128 MiB of HBM per device.

```python
import jax
import jax.numpy as jnp
from jax import lax

NX = 512
NY = 512
NZ = 256


def operator_pair(key, length):
    index = jnp.arange(length)
    offset = (index[None, :] - index[:, None]) % length

    def band(shift):
        return (offset == shift).astype(jnp.float32)
    ident = band(0)
    plus_one = band(1)
    minus_one = band(length - 1)
    plus_two = band(2)
    minus_two = band(length - 2)
    first_lhs = ident + (plus_one + minus_one) / 3.0
    first_rhs = 14.0 / 9.0 * (plus_one - minus_one) / 2.0 + 1.0 / 9.0 * (plus_two - minus_two) / 4.0
    second_lhs = ident + 2.0 / 11.0 * (plus_one + minus_one)
    second_rhs = 12.0 / 11.0 * (plus_one + minus_one - 2.0 * ident) + 3.0 / 11.0 * (plus_two + minus_two - 2.0 * ident) / 4.0
    first = jnp.linalg.solve(first_lhs, first_rhs)
    second = jnp.linalg.solve(second_lhs, second_rhs)
    keys = jax.random.split(key, 2)
    spacing = jnp.exp(jax.random.uniform(keys[0], (length,), jnp.float32, jnp.log(0.6), jnp.log(1.6)))
    extra = 0.5 * jax.random.normal(keys[1], (2, length, length), jnp.float32) / jnp.sqrt(length * 1.0)
    first = spacing[:, None] * first
    second = 0.25 * (spacing * spacing)[:, None] * second
    whole = jnp.stack([first, second]) + extra
    return jnp.clip(whole, -8.0, 8.0).astype(jnp.bfloat16)


def draw_x_operators(key, part):
    return operator_pair(jax.random.fold_in(key, 11), NX)


def draw_y_operators(key, part):
    return operator_pair(jax.random.fold_in(key, 23), NY)


def shard_levels(own_key, shape, shards, least, top_value):
    gain = 1.0
    for axis_at, shards_of in shards:
        draws = jax.random.uniform(jax.random.fold_in(jax.random.fold_in(own_key, 6), axis_at), (shards_of,), jnp.float32, least / len(shards), top_value / len(shards))
        gain = gain * jnp.repeat(jnp.exp(draws), shape[axis_at] // shards_of).reshape((-1,) + (1,) * (len(shape) - 1 - axis_at))
    return gain


def centred(own_key, dims, scale, limit, shards=(), dtype=jnp.bfloat16):
    array = scale * jax.random.normal(own_key, dims, jnp.float32)
    if shards:
        array = array * shard_levels(own_key, dims, shards, -0.22, 0.18)
    return jnp.clip(array, -limit, limit).astype(dtype)


def setup_inputs(seed: int = 0) -> dict:
    key_of = jax.random.split(jax.random.key(seed), 5)
    return {
        "species": centred(key_of[0], (3, NX, NY, NZ), 1.0, 6.0, ((1, 16), (2, 16))),
        "flow_field": centred(key_of[1], (3, NX, NY, NZ), 1.0, 6.0, ((1, 16), (2, 16))),
        "x_operators": draw_x_operators(jax.random.fold_in(key_of[4], 71), 0),
        "y_operators": draw_y_operators(jax.random.fold_in(key_of[4], 71), 0),
    }


def along_first(operators, field):
    ops = operators.astype(jnp.float32)
    values = field.astype(jnp.float32)
    first = jnp.einsum('ij,jyz->iyz', ops[0], values, precision=lax.Precision.HIGHEST)
    second = jnp.einsum('ij,jyz->iyz', ops[1], values, precision=lax.Precision.HIGHEST)
    return jnp.stack([first.astype(jnp.bfloat16), second.astype(jnp.bfloat16)])

def along_second(operators, field):
    ops = operators.astype(jnp.float32)
    values = field.astype(jnp.float32)
    first = jnp.einsum('ij,xjz->xiz', ops[0], values, precision=lax.Precision.HIGHEST)
    second = jnp.einsum('ij,xjz->xiz', ops[1], values, precision=lax.Precision.HIGHEST)
    return jnp.stack([first.astype(jnp.bfloat16), second.astype(jnp.bfloat16)])

def reference(species, flow_field, x_operators, y_operators):
    species_derivatives = lax.map(lambda field: along_first(x_operators, field), species)
    flow_derivatives = lax.map(lambda field: along_second(y_operators, field), flow_field)
    return (species_derivatives, flow_derivatives)
```

```python
import functools

import jax
import jax.numpy as jnp
from jax import lax
from jax.experimental import pallas as pl
from jax.experimental.pallas import tpu as pltpu
from jax.sharding import PartitionSpec as P


VMEM = pl.BlockSpec(memory_space=pltpu.VMEM)
RY, RC, RX = 4, 2, 2


def params(mib):
    return pltpu.CompilerParams(vmem_limit_bytes=mib << 20)


def cost(flops, size):
    return pl.CostEstimate(flops=flops, bytes_accessed=size, transcendentals=0)


def col_pack_kernel(x_ref, o_ref):
    n, fields, width = o_ref.shape[:3]
    for s in range(fields):
        for k in range(n):
            o_ref[k, s] = x_ref[s, k * width : (k + 1) * width]


def col_product_kernel(x_ref, a_ref, o_ref):
    n, _, width, wide, depth = x_ref.shape
    for w in range(width):
        x = x_ref[:, 0, w].reshape(n * wide, depth)
        for d in range(2):
            r = jnp.dot(a_ref[d], x, preferred_element_type=jnp.float32)
            o_ref[:, 0, d, w] = r.astype(o_ref.dtype).reshape(n, wide, depth)


def col_unpack_kernel(x_ref, o_ref):
    n, _, _, width = x_ref.shape[:4]
    for d in range(2):
        for k in range(n):
            o_ref[0, d, k * width : (k + 1) * width] = x_ref[k, 0, d]


def col_pack(x, n):
    fields, width, wide, depth = x.shape
    return pl.pallas_call(
        col_pack_kernel,
        out_shape=jax.ShapeDtypeStruct((n, fields, width // n, wide, depth), x.dtype),
        in_specs=[VMEM],
        out_specs=VMEM,
        compiler_params=params(16),
        cost_estimate=cost(0, 4 * x.size),
        name="col_pack",
    )(x)


def col_product(x, a):
    n, fields, width, wide, depth = x.shape
    return pl.pallas_call(
        col_product_kernel,
        grid=(fields,),
        out_shape=jax.ShapeDtypeStruct((n, fields, 2, width, wide, depth), x.dtype),
        in_specs=[
            pl.BlockSpec((n, 1, width, wide, depth), lambda s: (0, s, 0, 0, 0)),
            pl.BlockSpec(a.shape, lambda s: (0, 0, 0)),
        ],
        out_specs=pl.BlockSpec((n, 1, 2, width, wide, depth), lambda s: (0, s, 0, 0, 0, 0)),
        compiler_params=params(32),
        cost_estimate=cost(4 * x.size * a.shape[1], 6 * x.size + 2 * a.size),
        name="col_product",
    )(x, a)


def col_unpack(x):
    n, fields, _, width, wide, depth = x.shape
    return pl.pallas_call(
        col_unpack_kernel,
        grid=(fields,),
        out_shape=jax.ShapeDtypeStruct((fields, 2, n * width, wide, depth), x.dtype),
        in_specs=[pl.BlockSpec((n, 1, 2, width, wide, depth), lambda s: (0, s, 0, 0, 0, 0))],
        out_specs=pl.BlockSpec((1, 2, n * width, wide, depth), lambda s: (s, 0, 0, 0, 0)),
        compiler_params=params(16),
        cost_estimate=cost(0, 4 * x.size),
        name="col_unpack",
    )(x)


def swapped(v):
    return jnp.swapaxes(v.astype(jnp.float32), 0, 1).astype(v.dtype)


def row_pack_kernel(x_ref, *o_refs):
    y = lax.rem(lax.axis_index("row") // RC, RY)
    rows = o_refs[0].shape[1]
    for s in range(x_ref.shape[0]):
        for step in range(RY):
            first = pl.multiple_of(lax.rem(y + step, RY) * rows, rows)
            o_refs[step][s] = swapped(x_ref[s, :, pl.ds(first, rows), :])


def row_pack(x):
    fields, wide, width, depth = x.shape
    piece = jax.ShapeDtypeStruct((fields, width // RY, wide, depth), x.dtype)
    return pl.pallas_call(
        row_pack_kernel,
        out_shape=[piece] * RY,
        in_specs=[VMEM],
        out_specs=[VMEM] * RY,
        compiler_params=params(32),
        cost_estimate=cost(0, 4 * x.size),
        name="row_pack",
    )(x)


def row_product_kernel(*refs):
    pieces, a_ref, o_refs, x_buf = refs[:16], refs[16], refs[17:21], refs[21]
    fields, width, wide, depth = pieces[0].shape
    me = lax.axis_index("row")
    x, y, c = me // (RY * RC), lax.rem(me // RC, RY), lax.rem(me, RC)
    firsts = []
    for at in range(16):
        dc, dx, dy = at // 8, at // 4 % 2, at % 4
        sx = lax.rem(x + dx, RX)
        sc = lax.rem(c + dc, RC)
        source = (sx * RY + lax.rem(y + RY - dy, RY)) * RC + sc
        firsts.append(pl.multiple_of(source * wide, wide))
    own = []
    for dy in range(RY):
        target = (x * RY + lax.rem(y + dy, RY)) * RC + c
        own.append(pl.multiple_of(target * wide, wide))
    a = [jnp.concatenate([a_ref[d, pl.ds(f, wide), :] for f in own]) for d in range(2)]

    @pl.loop(0, fields)
    def _(s):
        for w in range(width):
            for at in range(16):
                x_buf[w % 2, pl.ds(firsts[at], wide), :] = pieces[at][s, w]
            b = x_buf[w % 2]
            for d in range(2):
                r = jnp.dot(a[d], b, preferred_element_type=jnp.float32)
                r = r.astype(jnp.bfloat16).reshape(RY, wide, depth)
                for dy in range(RY):
                    o_refs[dy][s, d, w] = r[dy]


def row_product(pieces, a):
    fields, width, wide, depth = pieces[0].shape
    full = a.shape[2]
    piece = jax.ShapeDtypeStruct((fields, 2, width, wide, depth), a.dtype)
    size = pieces[0].size
    return pl.pallas_call(
        row_product_kernel,
        out_shape=[piece] * RY,
        in_specs=[VMEM] * 17,
        out_specs=[VMEM] * RY,
        scratch_shapes=[pltpu.VMEM((2, full, depth), a.dtype)],
        compiler_params=params(48),
        cost_estimate=cost(4 * RY * wide * full * fields * width * depth, 2 * 24 * size),
        name="row_product",
    )(*pieces, a)


def row_unpack_kernel(q0, q1, q2, q3, o_ref):
    y = lax.rem(lax.axis_index("row") // RC, RY)
    rows = q0.shape[2]
    for step, q in enumerate((q0, q1, q2, q3)):
        first = pl.multiple_of(lax.rem(y + RY - step, RY) * rows, rows)
        for d in range(2):
            o_ref[0, d, :, pl.ds(first, rows), :] = swapped(q[0, d])


def row_unpack(pieces):
    fields, _, width, wide, depth = pieces[0].shape
    return pl.pallas_call(
        row_unpack_kernel,
        grid=(fields,),
        out_shape=jax.ShapeDtypeStruct((fields, 2, wide, RY * width, depth), pieces[0].dtype),
        in_specs=[pl.BlockSpec((1, 2, width, wide, depth), lambda s: (s, 0, 0, 0, 0))] * RY,
        out_specs=pl.BlockSpec((1, 2, wide, RY * width, depth), lambda s: (s, 0, 0, 0, 0)),
        compiler_params=params(32),
        cost_estimate=cost(0, 16 * pieces[0].size),
        name="row_unpack",
    )(*pieces)


def y_shift(step):
    return [(r, (r // 8) * 8 + ((r // 2 + step) % 4) * 2 + r % 2) for r in range(16)]


X_SWAP = [(r, r ^ 8) for r in range(16)]
CORE_SWAP = [(r, r ^ 1) for r in range(16)]


def body(species, flow_field, x_operators, y_operators):
    n = lax.axis_size("col")
    packed = col_pack(flow_field, n)
    arrived = lax.all_to_all(packed, "col", split_axis=0, concat_axis=0, tiled=True)

    species, packed = lax.optimization_barrier((species, packed))
    own = row_pack(species)
    own = [own[0]] + [lax.ppermute(own[k], "row", y_shift(k)) for k in range(1, RY)]
    pair = own + [lax.ppermute(p, "row", X_SWAP) for p in own]
    every = pair + [lax.ppermute(p, "row", CORE_SWAP) for p in pair]

    arrived, _ = lax.optimization_barrier((arrived, own))
    result = col_product(arrived, y_operators)
    returned = lax.all_to_all(result, "col", split_axis=0, concat_axis=0, tiled=True)

    out = row_product(every, x_operators)
    out = [out[0]] + [lax.ppermute(out[k], "row", y_shift(k)) for k in range(1, RY)]
    species_derivatives = row_unpack(out)
    flow_derivatives = col_unpack(returned)
    return (species_derivatives, flow_derivatives)


def solution(mesh):
    placed = (P(None, "row", "col", None), P(None, "row", "col", None), P(), P())
    return jax.shard_map(
        body,
        mesh=mesh,
        in_specs=placed,
        out_specs=(P(None, None, "row", "col", None), P(None, None, "row", "col", None)),
        check_vma=False,
    )
```
